32 devices in a mesh: rep: 4 (over x, y), dp: 8 (over z, core).
Axes of the slice: x: 2, y: 2, z: 4, core: 2. Of those that a mesh axis runs over, the one named last changes fastest.
Arguments:
- x: bfloat16 [32, 2048, 512], P(('rep', 'dp')), parts along dimension 0
- dy: bfloat16 [32, 2048, 512], P(('rep', 'dp')), parts along dimension 0
- wq: bfloat16 [2, 512, 768], P(None, 'dp')
- wk: bfloat16 [2, 512, 128], P(None, 'dp')
- wv: bfloat16 [2, 512, 128], P(None, 'dp')
- wo: bfloat16 [2, 768, 512], P(None, 'dp')
- w_gate: bfloat16 [2, 512, 2048], P(None, 'dp')
- w_up: bfloat16 [2, 512, 2048], P(None, 'dp')
- w_down: bfloat16 [2, 2048, 512], P(None, 'dp')
- m_wq: float32 [2, 512, 768], P(None, 'dp')
- m_wk: float32 [2, 512, 128], P(None, 'dp')
- m_wv: float32 [2, 512, 128], P(None, 'dp')
- m_wo: float32 [2, 768, 512], P(None, 'dp')
- m_w_gate: float32 [2, 512, 2048], P(None, 'dp')
- m_w_up: float32 [2, 512, 2048], P(None, 'dp')
- m_w_down: float32 [2, 2048, 512], P(None, 'dp')
- v_wq: float32 [2, 512, 768], P(None, 'dp')
- v_wk: float32 [2, 512, 128], P(None, 'dp')
- v_wv: float32 [2, 512, 128], P(None, 'dp')
- v_wo: float32 [2, 768, 512], P(None, 'dp')
- v_w_gate: float32 [2, 512, 2048], P(None, 'dp')
- v_w_up: float32 [2, 512, 2048], P(None, 'dp')
- v_w_down: float32 [2, 2048, 512], P(None, 'dp')
Outputs:
- output 1: bfloat16 [8, 512, 768], P('rep', 'dp'), parts along dimension 0
- output 2: bfloat16 [8, 512, 128], P('rep', 'dp'), parts along dimension 0
- output 3: bfloat16 [8, 512, 128], P('rep', 'dp'), parts along dimension 0
- output 4: bfloat16 [8, 768, 512], P('rep', 'dp'), parts along dimension 0
- output 5: bfloat16 [8, 512, 2048], P('rep', 'dp'), parts along dimension 0
- output 6: bfloat16 [8, 512, 2048], P('rep', 'dp'), parts along dimension 0
- output 7: bfloat16 [8, 2048, 512], P('rep', 'dp'), parts along dimension 0
- output 8: float32 [8, 512, 768], P('rep', 'dp'), parts along dimension 0
- output 9: float32 [8, 512, 128], P('rep', 'dp'), parts along dimension 0
- output 10: float32 [8, 512, 128], P('rep', 'dp'), parts along dimension 0
- output 11: float32 [8, 768, 512], P('rep', 'dp'), parts along dimension 0
- output 12: float32 [8, 512, 2048], P('rep', 'dp'), parts along dimension 0
- output 13: float32 [8, 512, 2048], P('rep', 'dp'), parts along dimension 0
- output 14: float32 [8, 2048, 512], P('rep', 'dp'), parts along dimension 0
- output 15: float32 [8, 512, 768], P('rep', 'dp'), parts along dimension 0
- output 16: float32 [8, 512, 128], P('rep', 'dp'), parts along dimension 0
- output 17: float32 [8, 512, 128], P('rep', 'dp'), parts along dimension 0
- output 18: float32 [8, 768, 512], P('rep', 'dp'), parts along dimension 0
- output 19: float32 [8, 512, 2048], P('rep', 'dp'), parts along dimension 0
- output 20: float32 [8, 512, 2048], P('rep', 'dp'), parts along dimension 0
- output 21: float32 [8, 2048, 512], P('rep', 'dp'), parts along dimension 0
There are 4 independent parts. The reference program is written for one: setup_inputs(seed, part) draws one part's arguments, and reference() takes and returns one part's arrays. A program takes and returns all parts, laid end to end along the dimension named above; an argument that names none is the same for every part.
All inputs are finite; a program needn't handle non-finite values.
Results may differ from the reference program's by a relative error of at most 0.0247.
Values are sent between devices in bfloat16 or wider.
A program may use at most 2 GiB of HBM per device.

```python
import jax
import jax.numpy as jnp
from jax import lax

SEQUENCES = 8
TOKENS = 2048
D = 512
HEADS = 6
KV_HEADS = 1
HEAD = 128
FF = 2048
LAYERS = 2
THETA = 10000
NAMES = ("wq", "wk", "wv", "wo", "w_gate", "w_up", "w_down")
SHAPES = {
    "wq": (LAYERS, D, HEADS * HEAD),
    "wk": (LAYERS, D, KV_HEADS * HEAD),
    "wv": (LAYERS, D, KV_HEADS * HEAD),
    "wo": (LAYERS, HEADS * HEAD, D),
    "w_gate": (LAYERS, D, FF),
    "w_up": (LAYERS, D, FF),
    "w_down": (LAYERS, FF, D),
}


def bump(key, n, height):
    away = (jnp.arange(n, dtype=jnp.int32) - jax.random.randint(key, (), 0, n, jnp.int32)) % n
    return jnp.where(away < n // 8, height, 1.0)


def together(key, own, strength):
    shared = jax.random.normal(key, own.shape[1:], jnp.float32)
    return (own + strength * shared) * lax.rsqrt(1 + strength * strength)


def setup_inputs(seed: int = 0, part: int = 0) -> dict:
    kx, kdy, ka, kb, kz, kf, kh, kl, *keys = jax.random.split(jax.random.key(seed), 8 + 3 * len(NAMES))
    kx, kdy, ka, kb = (jax.random.fold_in(k, part) for k in (kx, kdy, ka, kb))
    kw, km, kv = (keys[i::3] for i in range(3))
    shape = (SEQUENCES, TOKENS, D)
    much_x, much_dy = jax.random.uniform(kz, (2,), jnp.float32, 0.0, 1.0)
    loud = 2.0 ** jax.random.uniform(jax.random.fold_in(kz, 1), (), jnp.float32, -1.0, 2.0)
    layers = 2.0 ** jax.random.uniform(kl, (LAYERS, 1, 1), jnp.float32, -1.0, 1.0)
    times = {"wq": 1.0, "wk": 1.0, "wv": 2.0, "wo": layers, "w_gate": 1.0, "w_up": bump(kh, FF, 4.0), "w_down": layers}
    x = together(ka, jax.random.normal(kx, shape, jnp.float32), much_x) * bump(kf, D, 4.0)
    dy = together(kb, jax.random.normal(kdy, shape, jnp.float32), much_dy)
    drawn = {"x": x.astype(jnp.bfloat16), "dy": (loud * dy * (SEQUENCES * TOKENS) ** -0.5).astype(jnp.bfloat16)}
    for key, name in zip(kw, NAMES, strict=True):
        drawn[name] = (jax.random.normal(key, SHAPES[name], jnp.float32) * SHAPES[name][1] ** -0.5 * times[name]).astype(jnp.bfloat16)
    for key, name in zip(km, NAMES, strict=True):
        drawn[f"m_{name}"] = 0.1 * jax.random.normal(key, SHAPES[name], jnp.float32)
    for key, name in zip(kv, NAMES, strict=True):
        drawn[f"v_{name}"] = jax.random.uniform(key, SHAPES[name], jnp.float32, 0.02, 0.06)
    return drawn


def matmul(a, w):
    return jnp.dot(a, w, preferred_element_type=jnp.float32).astype(jnp.bfloat16)


def normed(h):
    wide = h.astype(jnp.float32)
    scale = lax.rsqrt(jnp.mean(wide**2, -1, keepdims=True) + 1e-6)
    return (wide * scale).astype(jnp.bfloat16)


def turned(t, theta):
    half = t.shape[-1] // 2
    angle = jnp.arange(t.shape[0], dtype=jnp.float32)[:, None] * theta ** (-jnp.arange(half, dtype=jnp.float32) / half)
    cos, sin = jnp.cos(angle)[:, None], jnp.sin(angle)[:, None]
    a, b = t[..., :half].astype(jnp.float32), t[..., half:].astype(jnp.float32)
    return jnp.concatenate([a * cos - b * sin, b * cos + a * sin], -1).astype(jnp.bfloat16)


def seen_by(q, k, v):
    tokens, kv = q.shape[0], k.shape[1]
    q = q.reshape(tokens, kv, -1, q.shape[-1])
    scores = jnp.einsum("tgsd,ugd->gstu", q.astype(jnp.float32), k.astype(jnp.float32)) * q.shape[-1] ** -0.5
    place = jnp.arange(tokens)
    weights = jax.nn.softmax(jnp.where(place[:, None] >= place, scores, -jnp.inf), -1).astype(jnp.bfloat16)
    return jnp.einsum("gstu,ugd->tgsd", weights.astype(jnp.float32), v.astype(jnp.float32)).astype(jnp.bfloat16).reshape(tokens, -1)


def layer(h, w):
    a = normed(h)
    q, k = (turned(matmul(a, w[name]).reshape(h.shape[0], -1, HEAD), THETA) for name in ("wq", "wk"))
    h = h + matmul(seen_by(q, k, matmul(a, w["wv"]).reshape(h.shape[0], -1, HEAD)), w["wo"])
    b = normed(h)
    gate = jnp.dot(b, w["w_gate"], preferred_element_type=jnp.float32)
    up = jnp.dot(b, w["w_up"], preferred_element_type=jnp.float32)
    return h + matmul((jax.nn.silu(gate) * up).astype(jnp.bfloat16), w["w_down"])


def adamw(w, m, v, g):
    m = 0.9 * m + 0.1 * g
    v = 0.95 * v + 0.05 * g * g
    step = m * lax.rsqrt(v + 1e-8) + 0.1 * w
    return (w - 0.02 * step).astype(jnp.bfloat16), m, v


def clipped(gradients, sum_of_squares, count):
    factor = jnp.minimum(1.0, 0.5 * lax.rsqrt(sum_of_squares / count + 1e-30))
    return [g * factor for g in gradients]


def stack(weights, h):
    return lax.scan(lambda h, w: (layer(h, w), None), h, weights)[0]


def reference(x, dy, wq, wk, wv, wo, w_gate, w_up, w_down, m_wq, m_wk, m_wv, m_wo, m_w_gate, m_w_up, m_w_down, v_wq, v_wk, v_wv, v_wo, v_w_gate, v_w_up, v_w_down):
    weights = dict(zip(NAMES, (wq, wk, wv, wo, w_gate, w_up, w_down), strict=True))

    def take(so_far, sequence):
        h, by_y = sequence
        _, back = jax.vjp(stack, weights, h)
        by_weights, by_h = back(by_y)
        return jax.tree.map(lambda total, term: total + term.astype(jnp.float32), so_far, by_weights), by_h

    none_yet = {name: jnp.zeros(w.shape, jnp.float32) for name, w in weights.items()}
    by_weights, by_x = lax.scan(take, none_yet, (x, dy))
    gradients = [by_weights[name].astype(jnp.bfloat16).astype(jnp.float32) for name in NAMES]
    gradients = clipped(gradients, sum(jnp.sum(g * g) for g in gradients), sum(g.size for g in gradients))
    first = (m_wq, m_wk, m_wv, m_wo, m_w_gate, m_w_up, m_w_down)
    second = (v_wq, v_wk, v_wv, v_wo, v_w_gate, v_w_up, v_w_down)
    new = [adamw(weights[name].astype(jnp.float32), m, v, g) for name, m, v, g in zip(NAMES, first, second, gradients, strict=True)]
    return tuple(one[which] for which in range(3) for one in new)
```

```python
import functools
import jax
import jax.numpy as jnp
from jax import lax
from jax.experimental import pallas as pl
from jax.experimental.pallas import tpu as pltpu
from jax.sharding import PartitionSpec as P

BF, F32 = jnp.bfloat16, jnp.float32
HEAD, THETA = 128, 10000
LOG2E = 1.4426950408889634
NEG = -1e30
LIMIT = 62 * 2**20
TILE = 512
SUB = 256
LAG1, LAG2, FKEYS, FCOLS = 3, 3, 512, 512
BLAG1, BLAG2, BKEYS, BCOLS = 2, 2, 512, 256
MLAG, FPART, MLAG1 = 1, 256, 1


def _mm(a, b, ca=1, cb=0):
    return lax.dot_general(a, b, (((ca,), (cb,)), ((), ())), preferred_element_type=F32)


def _norm(x):
    s = lax.rsqrt(jnp.mean(x * x, -1, keepdims=True) + 1e-6)
    return (x * s).astype(BF), s


def _norm_bwd(x, s, dn):
    dn = dn.astype(F32)
    return (s * dn - x * (s * s * s * jnp.mean(dn * x, -1, keepdims=True))).astype(BF)


def _plus(a, b):
    return (a.astype(F32) + b.astype(F32)).astype(BF)


def _at(i, size):
    return pl.ds(pl.multiple_of(i * size, size), size)


def _attend_fwd(h_ref, wqkv_ref, wo_ref, cos_ref, sin_ref, qt_ref, k_ref, v_ref, kt_ref, ot_ref, lse_ref, h1_ref, wt_s, vt_s, top_s, mix_s,
                *, heads):
    i = pl.program_id(0)
    n, half = TILE, HEAD // 2
    e = HEAD**-0.5 * LOG2E
    cols = heads * n

    @pl.when(i == 0)
    def _():
        wt_s[...] = wqkv_ref[...].T
        vt_s[HEAD:, :] = jnp.ones((16, vt_s.shape[1]), BF)

    h = h_ref[...]
    a, _ = _norm(h.astype(F32))
    qkv = _mm(wt_s[...], a, 1, 1).astype(BF)
    cos, sin = cos_ref[...], sin_ref[...]

    def turned(t):
        x, y = t[:half].astype(F32), t[half:].astype(F32)
        return jnp.concatenate([x * cos - y * sin, y * cos + x * sin], 0).astype(BF)

    for m in range(heads):
        qt_ref[m * HEAD : (m + 1) * HEAD, :] = turned(qkv[m * HEAD : (m + 1) * HEAD])
    kt = turned(qkv[heads * HEAD : (heads + 1) * HEAD])
    vt = qkv[(heads + 1) * HEAD :]
    here = _at(i, n)
    kt_ref[...] = kt
    k_ref[here, :] = kt.T
    v_ref[here, :] = vt.T
    vt_s[:HEAD, here] = vt
    top_s[...] = jnp.full(top_s.shape, NEG, F32)
    mix_s[...] = jnp.zeros_like(mix_s)

    def block(at, low, wide):
        keys = k_ref[at, :]
        values = vt_s[:, at]
        pieces = [(m, p) for m in range(heads) for p in range(0, n, wide) if low is None or p >= low]
        scores, weights = {}, {}
        for z in range(len(pieces) + LAG1 + LAG2):
            if z < len(pieces):
                m, p = pieces[z]
                scores[z] = _mm(keys, qt_ref[m * HEAD : (m + 1) * HEAD, p : p + wide])
            y = z - LAG1
            if 0 <= y < len(pieces):
                m, p = pieces[y]
                c = slice(m * n + p, m * n + p + wide)
                s = scores.pop(y)
                if p == low:
                    s = jnp.where(lax.broadcasted_iota(jnp.int32, s.shape, 1) >= lax.broadcasted_iota(jnp.int32, s.shape, 0), s, 2 * NEG)
                old = top_s[0:1, c]
                top = jnp.maximum(old, s.max(0, keepdims=True))
                top_s[0:1, c] = top
                weights[y] = jnp.exp2((s - top) * e).astype(BF), jnp.exp2((old - top) * e)
            y -= LAG2
            if 0 <= y < len(pieces):
                m, p = pieces[y]
                c = slice(m * n + p, m * n + p + wide)
                w, keep = weights.pop(y)
                mix_s[:, c] = mix_s[:, c] * keep + _mm(values, w)

    lax.fori_loop(0, i * (n // FKEYS), lambda j, _: block(_at(j, FKEYS), None, FCOLS), None)
    for low in range(0, n, SUB):
        block(pl.ds(pl.multiple_of(i * n + low, SUB), SUB), low, SUB)
    for m in range(heads):
        c = slice(m * n, (m + 1) * n)
        total = mix_s[HEAD : HEAD + 1, c]
        ot_ref[m * HEAD : (m + 1) * HEAD, :] = (mix_s[:HEAD, c] * (1 / total)).astype(BF)
        lse_ref[m : m + 1, :] = top_s[0:1, c] + jnp.log2(total) * (1 / e)
    h1_ref[...] = _plus(h, _mm(ot_ref[...], wo_ref[...], 0, 0).astype(BF))


def attend_fwd(h, wqkv, wo, cost, sint):
    t, d = h.shape
    heads = wo.shape[0] // HEAD
    n = TILE
    w = wqkv.shape[1]
    whole = lambda *s: pl.BlockSpec(s, lambda i: (0,) * len(s))
    col = lambda r: pl.BlockSpec((r, n), lambda i: (0, i))
    row = lambda c: pl.BlockSpec((n, c), lambda i: (i, 0))
    sd = jax.ShapeDtypeStruct
    return pl.pallas_call(
        functools.partial(_attend_fwd, heads=heads),
        grid=(t // n,),
        in_specs=[row(d), whole(d, w), whole(heads * HEAD, d), col(HEAD // 2), col(HEAD // 2)],
        out_specs=[col(heads * HEAD), whole(t, HEAD), whole(t, HEAD), col(HEAD), col(heads * HEAD), col(8), row(d)],
        out_shape=[sd((heads * HEAD, t), BF), sd((t, HEAD), BF), sd((t, HEAD), BF), sd((HEAD, t), BF), sd((heads * HEAD, t), BF),
                   sd((8, t), F32), sd((t, d), BF)],
        scratch_shapes=[pltpu.VMEM((w, d), BF), pltpu.VMEM((HEAD + 16, t), BF), pltpu.VMEM((8, heads * n), F32),
                        pltpu.VMEM((HEAD + 16, heads * n), F32)],
        compiler_params=pltpu.CompilerParams(dimension_semantics=("arbitrary",), vmem_limit_bytes=LIMIT),
        cost_estimate=pl.CostEstimate(flops=2 * t * d * (w + heads * HEAD) + 2 * heads * t * t * HEAD, transcendentals=heads * t * t // 2,
                                      bytes_accessed=16 * t * d),
        name="attend_fwd",
    )(h, wqkv, wo, cost, sint)


def _mlp_fwd(h_ref, wg_ref, wu_ref, wd_ref, out_ref, gate_ref, up_ref, b_s, y_s):
    c = pl.program_id(0)
    t, n = h_ref.shape[0], TILE

    @pl.when(c == 0)
    def _():
        for at in range(0, t, n):
            b_s[at : at + n, :], _ = _norm(h_ref[at : at + n, :].astype(F32))

    raw = {}
    for z in range(t // n + MLAG):
        if z < t // n:
            b = b_s[z * n : (z + 1) * n, :]
            raw[z] = _mm(b, wg_ref[...]), _mm(b, wu_ref[...])
        y = z - MLAG
        if 0 <= y < t // n:
            at = slice(y * n, (y + 1) * n)
            gate, up = raw.pop(y)
            gate_ref[at, :] = gate
            up_ref[at, :] = up
            more = _mm((gate * jax.nn.sigmoid(gate) * up).astype(BF), wd_ref[...])
            y_s[at, :] = jnp.where(c == 0, 0.0, y_s[at, :]) + more

    @pl.when(c == pl.num_programs(0) - 1)
    def _():
        for at in range(0, t, n):
            out_ref[at : at + n, :] = _plus(h_ref[at : at + n, :], y_s[at : at + n, :].astype(BF))


def mlp_fwd(h, wgu, wd):
    t, d = h.shape
    ff = wd.shape[0]
    n = FPART
    once = lambda *s: pl.BlockSpec(s, lambda i: (0,) * len(s), pipeline_mode=pl.Buffered(1))
    sd = jax.ShapeDtypeStruct
    return pl.pallas_call(
        _mlp_fwd,
        grid=(ff // n,),
        in_specs=[once(t, d), pl.BlockSpec((d, n), lambda i: (0, i)), pl.BlockSpec((d, n), lambda i: (0, i + ff // n)),
                  pl.BlockSpec((n, d), lambda i: (i, 0))],
        out_specs=[once(t, d), pl.BlockSpec((t, n), lambda i: (0, i)), pl.BlockSpec((t, n), lambda i: (0, i))],
        out_shape=[sd((t, d), BF), sd((t, ff), F32), sd((t, ff), F32)],
        scratch_shapes=[pltpu.VMEM((t, d), BF), pltpu.VMEM((t, d), F32)],
        compiler_params=pltpu.CompilerParams(dimension_semantics=("arbitrary",), vmem_limit_bytes=LIMIT),
        cost_estimate=pl.CostEstimate(flops=6 * t * d * ff, transcendentals=t * ff, bytes_accessed=8 * t * ff),
        name="mlp_fwd",
    )(h, wgu, wgu, wd)


def _mlp_bwd(h_ref, dy_ref, *rest, saved):
    (gate_ref, up_ref), rest = (rest[:2], rest[2:]) if saved else ((None, None), rest)
    wg_ref, wu_ref, wd_ref, dh_ref, g_ref, b_s, bt_s, dyt_s, db_s, dg_s, du_s, act_s, og_s, ou_s, od_s, sem = rest
    c = pl.program_id(0)
    t, d = h_ref.shape
    n = TILE
    blocks = g_ref.shape[0]
    r = d // blocks
    tiles = range(t // n)

    @pl.when(c == 0)
    def _():
        for z in tiles:
            at = slice(z * n, (z + 1) * n)
            b, _ = _norm(h_ref[at, :].astype(F32))
            b_s[at, :], bt_s[:, at], dyt_s[:, at] = b, b.T, dy_ref[at, :].T

    raw = {}
    for z in range(len(tiles) + MLAG1):
        if z < len(tiles):
            at = slice(z * n, (z + 1) * n)
            raw[z] = _mm(dy_ref[at, :], wd_ref[...], 1, 1), *(() if saved else (_mm(b_s[at, :], wg_ref[...]), _mm(b_s[at, :], wu_ref[...])))
        y = z - MLAG1
        if 0 <= y < len(tiles):
            at = slice(y * n, (y + 1) * n)
            dact, *both = raw.pop(y)
            gate, up = both if both else (gate_ref[at, :], up_ref[at, :])
            dact = dact.astype(BF).astype(F32)
            sig = jax.nn.sigmoid(gate)
            silu = gate * sig
            act_s[at, :] = (silu * up).astype(BF)
            du_s[at, :] = (dact * silu).astype(BF)
            dg_s[at, :] = (dact * up * (sig + silu * (1 - sig))).astype(BF)

    for z in tiles:
        at = slice(z * n, (z + 1) * n)
        more = _mm(dg_s[at, :], wg_ref[...], 1, 1) + _mm(du_s[at, :], wu_ref[...], 1, 1)
        db_s[at, :] = jnp.where(c == 0, 0.0, db_s[at, :]) + more

    per = od_s.shape[2]

    def out(step):
        slot = lax.rem(step, 2)
        cut = pl.num_programs(0)
        where = (g_ref.at[:, _at(step, r), :], g_ref.at[:, _at(cut + step, r), :],
                 g_ref.at[pl.ds(step * (d // per), d // per), pl.ds(2 * r * STEPS, per), :])
        return [pltpu.make_async_copy(b.at[slot], w, sem.at[slot, m]) for m, (b, w) in enumerate(zip((og_s, ou_s, od_s), where))]

    @pl.when(c >= 2)
    def _():
        for copy in out(c - 2):
            copy.wait()

    slot = lax.rem(c, 2)
    og_s[slot] = _mm(bt_s[...], dg_s[...]).astype(BF).reshape(blocks, r, d)
    ou_s[slot] = _mm(bt_s[...], du_s[...]).astype(BF).reshape(blocks, r, d)
    od_s[slot] = _mm(dyt_s[...], act_s[...]).astype(BF).T.reshape(d // per, per, d)
    for copy in out(c):
        copy.start()

    @pl.when(c == pl.num_programs(0) - 1)
    def _():
        for z in tiles:
            at = slice(z * n, (z + 1) * n)
            x = h_ref[at, :].astype(F32)
            s = lax.rsqrt(jnp.mean(x * x, -1, keepdims=True) + 1e-6)
            dh_ref[at, :] = _plus(dy_ref[at, :], _norm_bwd(x, s, db_s[at, :].astype(BF)))
        for step in (c - 1, c):
            for copy in out(step):
                copy.wait()


STEPS = 4


def mlp_bwd(h, dy, wgu, wd, saved, blocks):
    t, d = h.shape
    ff = wd.shape[0]
    n, per = d, ff // blocks
    rows = 3 * per
    once = lambda *s: pl.BlockSpec(s, lambda i: (0,) * len(s), pipeline_mode=pl.Buffered(1))
    cols = lambda r, skip=0: pl.BlockSpec((r, n), lambda i: (0, i + skip))
    sd = jax.ShapeDtypeStruct
    return pl.pallas_call(
        functools.partial(_mlp_bwd, saved=bool(saved)),
        grid=(ff // n,),
        in_specs=[once(t, d), once(t, d)] + [cols(t)] * len(saved) + [cols(d), cols(d, ff // n), pl.BlockSpec((n, d), lambda i: (i, 0))],
        out_specs=[once(t, d), pl.BlockSpec(memory_space=pl.ANY)],
        out_shape=[sd((t, d), BF), sd((blocks, rows, d), BF)],
        scratch_shapes=[pltpu.VMEM((t, d), BF), pltpu.VMEM((d, t), BF), pltpu.VMEM((d, t), BF), pltpu.VMEM((t, d), F32)]
        + [pltpu.VMEM((t, n), BF)] * 3 + [pltpu.VMEM((2, blocks, d // blocks, d), BF)] * 2 + [pltpu.VMEM((2, n // per, per, d), BF),
                                                                                          pltpu.SemaphoreType.DMA((2, 3))],
        compiler_params=pltpu.CompilerParams(dimension_semantics=("arbitrary",), vmem_limit_bytes=LIMIT),
        cost_estimate=pl.CostEstimate(flops=(12 if saved else 16) * t * d * ff, transcendentals=t * ff, bytes_accessed=8 * t * ff),
        name="mlp_bwd" if saved else "mlp_both",
    )(h, dy, *saved, wgu, wgu, wd)


def _attend_bwd(h_ref, dh1_ref, qt_ref, ot_ref, lse_ref, k_ref, v_ref, kt_ref, wqkv_ref, wo_ref, cos_ref, sin_ref, *rest, heads, need):
    (dh_ref,), rest = (rest[:1], rest[1:]) if need else ((None,), rest)
    g_ref, ka_s, va_s, qa_s, da_s, dk_s, dv_s, dq_s, dt_s, dw_s, dwo_s = rest
    step = pl.program_id(0)
    i = pl.num_programs(0) - 1 - step
    n, half = TILE, HEAD // 2
    e = HEAD**-0.5 * LOG2E
    t, d = k_ref.shape[0], h_ref.shape[1]

    @pl.when(step == 0)
    def _():
        less = jnp.where(lax.broadcasted_iota(jnp.int32, (t, HEAD), 1) < 3, -1.0, 0.0).astype(BF)
        ka_s[:, :HEAD], ka_s[:, HEAD:] = k_ref[...], less
        va_s[:, :HEAD], va_s[:, HEAD:] = v_ref[...], less
        for s in (dk_s, dv_s, dw_s, dwo_s):
            s[...] = jnp.zeros_like(s)

    def thirds(x):
        a = x.astype(BF)
        r = x - a.astype(F32)
        b = r.astype(BF)
        c = (r - b.astype(F32)).astype(BF)
        at = lax.broadcasted_iota(jnp.int32, (HEAD, n), 0)
        wide = lambda y: jnp.broadcast_to(y.astype(F32), (HEAD, n))
        return jnp.where(at == 0, wide(a), jnp.where(at == 1, wide(b), jnp.where(at == 2, wide(c), 0.0))).astype(BF)

    dh1 = dh1_ref[...]
    dot = _mm(wo_ref[...], dh1, 1, 1).astype(BF)
    for m in range(heads):
        r, c = slice(m * HEAD, (m + 1) * HEAD), slice(m * n, (m + 1) * n)
        qa_s[:HEAD, c] = qt_ref[r, :]
        qa_s[HEAD:, c] = thirds(lse_ref[m : m + 1, :])
        da_s[:HEAD, c] = dot[r]
        da_s[HEAD:, c] = thirds((dot[r].astype(F32) * ot_ref[r, :].astype(F32)).sum(0, keepdims=True))
    dwo_s[...] += _mm(ot_ref[...], dh1)
    dq_s[...] = jnp.zeros_like(dq_s)

    def block(at, low, wide):
        keys, values, kt = ka_s[at, :], va_s[at, :], kt_ref[:, at]
        pieces = [(m, p) for m in range(heads) for p in range(0, n, wide) if low is None or p >= low]
        dv = dk = None
        raw, ready = {}, {}
        for z in range(len(pieces) + BLAG1 + BLAG2):
            if z < len(pieces):
                m, p = pieces[z]
                c = slice(m * n + p, m * n + p + wide)
                raw[z] = _mm(keys, qa_s[:, c]), _mm(values, da_s[:, c])
            y = z - BLAG1
            if 0 <= y < len(pieces):
                m, p = pieces[y]
                s, dp = raw.pop(y)
                w = jnp.exp2(s * e)
                if p == low:
                    w = jnp.where(lax.broadcasted_iota(jnp.int32, w.shape, 1) >= lax.broadcasted_iota(jnp.int32, w.shape, 0), w, 0.0)
                ready[y] = w.astype(BF), (w * dp).astype(BF)
            y -= BLAG2
            if 0 <= y < len(pieces):
                m, p = pieces[y]
                c = slice(m * n + p, m * n + p + wide)
                w, ds = ready.pop(y)
                a, b = _mm(w, da_s[:HEAD, c], 1, 1), _mm(ds, qa_s[:HEAD, c], 1, 1)
                dv, dk = (a, b) if dv is None else (dv + a, dk + b)
                dq_s[:, c] += _mm(kt, ds)
        dv_s[at, :] += dv
        dk_s[at, :] += dk

    lax.fori_loop(0, i * (n // BKEYS), lambda j, _: block(_at(j, BKEYS), None, BCOLS), None)
    for low in range(0, n, SUB):
        block(pl.ds(pl.multiple_of(i * n + low, SUB), SUB), low, SUB)

    cos, sin = cos_ref[...], sin_ref[...]

    def back(t):
        x, y = t[:half].astype(F32), t[half:].astype(F32)
        return jnp.concatenate([x * cos + y * sin, y * cos - x * sin], 0).astype(BF)

    here = _at(i, n)
    for m in range(heads):
        dt_s[m * HEAD : (m + 1) * HEAD, :] = back((dq_s[:, m * n : (m + 1) * n] * HEAD**-0.5).astype(BF))
    dt_s[heads * HEAD : (heads + 1) * HEAD, :] = back((dk_s[here, :] * HEAD**-0.5).astype(BF).T)
    dt_s[(heads + 1) * HEAD :, :] = dv_s[here, :].astype(BF).T
    x = h_ref[...].astype(F32)
    a, s = _norm(x)
    dw_s[...] += _mm(dt_s[...], a)
    if need:
        da = _mm(wqkv_ref[...], dt_s[...]).astype(BF).T
        dh_ref[...] = _plus(dh1, _norm_bwd(x, s, da))

    @pl.when(step == pl.num_programs(0) - 1)
    def _():
        blocks = g_ref.shape[0]
        r, cut, per = d // blocks, dw_s.shape[0] // d, dwo_s.shape[0] // blocks
        for c in range(cut):
            w = dw_s[c * d : (c + 1) * d, :].T.astype(BF)
            for k in range(blocks):
                g_ref[k, c * r : (c + 1) * r, :] = w[k * r : (k + 1) * r]
        for k in range(blocks):
            g_ref[k, cut * r :, :] = dwo_s[k * per : (k + 1) * per, :].astype(BF)


def attend_bwd(h, dh1, kept, wqkv, wo, cost, sint, need, blocks):
    qt, k, v, kt, ot, lse = kept
    t, d = h.shape
    heads = wo.shape[0] // HEAD
    n, w = TILE, wqkv.shape[1]
    last = t // n - 1
    whole = lambda *s: pl.BlockSpec(s, lambda i: (0,) * len(s))
    col = lambda r: pl.BlockSpec((r, n), lambda i: (0, last - i))
    row = lambda c: pl.BlockSpec((n, c), lambda i: (last - i, 0))
    sd = jax.ShapeDtypeStruct
    rows = (w * d + heads * HEAD * d) // d // blocks
    got = pl.pallas_call(
        functools.partial(_attend_bwd, heads=heads, need=need),
        grid=(t // n,),
        in_specs=[row(d), row(d), col(heads * HEAD), col(heads * HEAD), col(8), whole(t, HEAD), whole(t, HEAD), whole(HEAD, t),
                  whole(d, w), whole(heads * HEAD, d), col(HEAD // 2), col(HEAD // 2)],
        out_specs=[row(d)] * need + [pl.BlockSpec((blocks, rows, d), lambda i: (0, 0, 0), pipeline_mode=pl.Buffered(1))],
        out_shape=[sd((t, d), BF)] * need + [sd((blocks, rows, d), BF)],
        scratch_shapes=[pltpu.VMEM((t, 2 * HEAD), BF), pltpu.VMEM((t, 2 * HEAD), BF), pltpu.VMEM((2 * HEAD, heads * n), BF),
                        pltpu.VMEM((2 * HEAD, heads * n), BF), pltpu.VMEM((t, HEAD), F32), pltpu.VMEM((t, HEAD), F32),
                        pltpu.VMEM((HEAD, heads * n), F32), pltpu.VMEM((w, n), BF), pltpu.VMEM((w, d), F32), pltpu.VMEM((heads * HEAD, d), F32)],
        compiler_params=pltpu.CompilerParams(dimension_semantics=("arbitrary",), vmem_limit_bytes=LIMIT),
        cost_estimate=pl.CostEstimate(flops=4 * t * d * (w + heads * HEAD) + 5 * heads * t * t * HEAD, transcendentals=heads * t * t // 2,
                                      bytes_accessed=16 * t * d),
        name="attend_bwd",
    )(h, dh1, qt, ot, lse, k, v, kt, wqkv, wo, cost, sint)
    return got if need else (None, got[0])


def tables(t):
    half = HEAD // 2
    angle = jnp.arange(t, dtype=F32)[None, :] * (THETA ** (-jnp.arange(half, dtype=F32) / half))[:, None]
    return jnp.cos(angle), jnp.sin(angle)

NAMES = ("wq", "wk", "wv", "wo", "w_gate", "w_up", "w_down")


def adamw(w, m, v, g):
    m = 0.9 * m + 0.1 * g
    v = 0.95 * v + 0.05 * g * g
    step = m * lax.rsqrt(v + 1e-8) + 0.1 * w
    return (w - 0.02 * step).astype(BF), m, v


def solution(mesh):
    blocks = mesh.shape["dp"]

    def gathered(weights, number):
        wq, wk, wv, wo, gate, up, down = (w[number] for w in weights)
        d = wo.shape[1]
        qkv = jnp.concatenate([wq, wk, wv], 1)
        r, cut = qkv.shape[0], qkv.shape[1] // d
        packed = jnp.concatenate([qkv[:, c * d : (c + 1) * d] for c in range(cut)] + [wo], 0)
        one = lax.all_gather(packed, "dp")
        two = lax.all_gather(jnp.concatenate([gate, up], 1), "dp", tiled=True)
        three = lax.all_gather(down, "dp", tiled=True)
        wqkv = one[:, : cut * r].reshape(blocks, cut, r, d).transpose(0, 2, 1, 3).reshape(blocks * r, cut * d)
        return wqkv, one[:, cut * r :].reshape(-1, d), two, three

    def scattered(g):
        return lax.psum_scatter(g, "dp", scatter_dimension=0, tiled=True)[0]

    def step(x, dy, *arrays):
        weights, m, v = (arrays[i : i + 7] for i in (0, 7, 14))
        layers = weights[0].shape[0]
        h, dh = x[0], dy[0]
        cost, sint = tables(h.shape[0])
        held, kept = [gathered(weights, number) for number in range(layers)], []
        for number in range(layers):
            wqkv, wo, wgu, wd = held[number]
            *att, h1 = attend_fwd(h, wqkv, wo, cost, sint)
            kept.append([h, h1, att, ()])
            if number < layers - 1:
                h, *kept[-1][3] = mlp_fwd(h1, wgu, wd)
        mine = [None] * layers
        for number in reversed(range(layers)):
            wqkv, wo, wgu, wd = held[number]
            h, h1, att, saved = kept[number]
            dh, g_mlp = mlp_bwd(h1, dh, wgu, wd, saved, blocks)
            g_mlp = scattered(g_mlp)
            dh, g_att = attend_bwd(h, dh, att, wqkv, wo, cost, sint, number > 0, blocks)
            g_att = scattered(g_att)
            d = h.shape[1]
            r = d // blocks
            wide = lambda g: g.reshape(-1, r, d).transpose(1, 0, 2).reshape(r, -1)
            nq, nf = wqkv.shape[1] // d * r, wd.shape[0] // d * r
            qkv = wide(g_att[:nq])
            nh = wo.shape[0]
            mine[number] = [qkv[:, :nh], qkv[:, nh : nh + HEAD], qkv[:, nh + HEAD :], g_att[nq:], wide(g_mlp[:nf]), wide(g_mlp[nf : 2 * nf]), g_mlp[2 * nf :]]
        gradients = [jnp.stack([mine[number][i] for number in range(layers)]).astype(F32) for i in range(7)]
        squares = lax.psum(sum(jnp.sum(g * g) for g in gradients), "dp")
        count = blocks * sum(g.size for g in gradients)
        factor = jnp.minimum(1.0, 0.5 * lax.rsqrt(squares / count + 1e-30))
        new = [adamw(w.astype(F32), m, v, g * factor) for w, m, v, g in zip(weights, m, v, gradients, strict=True)]
        return tuple(one[which] for which in range(3) for one in new)

    states, cut = P(("rep", "dp"), None, None), P(None, "dp", None)
    return jax.shard_map(
        step,
        mesh=mesh,
        in_specs=(states, states) + (cut,) * 21,
        out_specs=(P("rep", "dp", None),) * 21,
        check_vma=False,
    )
```
